32 devices in a mesh: depth: 4 (over y, x), screen: 8 (over z, core).
Axes of the slice: x: 2, y: 2, z: 4, core: 2. Of those that a mesh axis runs over, the one named last changes fastest.
Arguments:
- voxel_bins: int32 [32, 256, 2048], P('depth', None, 'screen'), may hold values from 0 to 255
- colors: bfloat16 [3, 256], replicated, may hold values from 0 to 2
- opacity: bfloat16 [256], replicated, may hold values from 0 to 1
- slab_order: int32 [8, 4], replicated, may hold values from 0 to 3, each once within a row
Outputs:
- image: float32 [4, 256, 2048], P(None, ('depth', 'screen'))
The draws below stay inside these ranges and needn't reach their ends.
Inputs may be any that keep to these rules, and one draw needn't show every extreme that they name: `slab_order`: every row is a permutation of 0 to 3.
All inputs are finite; a program needn't handle non-finite values.
Results may differ from the reference program's by a relative error of at most 0.0003.
Values sent between devices are 32-bit elements; how exact they have to be, the bound alone decides.
A program may use at most 64 MiB of HBM per device.

```python
import jax
import jax.numpy as jnp
from jax import lax

NBINS = 256
IMG_H = 256
SAMPLES = 32
IMG_W = 2048
DEPTHS = 4
TILES = 8


def place_ends(result, own_key, least, largest):
    extent = result.shape
    index_at = [jax.random.randint(jax.random.fold_in(own_key, axis), (), 0, extent[axis]) for axis in range(len(extent))]
    result = result.at[tuple(index_at)].set(least)
    longest = extent.index(max(extent))
    index_at[longest] = (index_at[longest] + 1) % extent[longest]
    return result.at[tuple(index_at)].set(largest)


def setup_inputs(seed: int = 0) -> dict:
    arg_keys = jax.random.split(jax.random.key(seed), 5)
    voxel_bins = place_ends(jax.random.randint(arg_keys[0], (SAMPLES, IMG_H, IMG_W), 0, NBINS), jax.random.fold_in(arg_keys[0], 1), 0, NBINS - 1).astype(jnp.int32)
    colors = jnp.clip(jax.random.uniform(arg_keys[1], (3, NBINS), jnp.float32, 0.0, 2.0), 0.0, 2.0).astype(jnp.bfloat16)
    opacity = jnp.clip(jax.random.uniform(arg_keys[2], (NBINS,), jnp.float32, 0.0, 1.0), 0.0, 1.0).astype(jnp.bfloat16)
    slab_order = jax.vmap(lambda own: jax.random.permutation(own, DEPTHS))(jax.random.split(arg_keys[3], TILES)).reshape((TILES, DEPTHS)).astype(jnp.int32)
    return dict(voxel_bins=voxel_bins, colors=colors, opacity=opacity, slab_order=slab_order)


def reference(voxel_bins, colors, opacity, slab_order):
    table = jnp.concatenate([colors, opacity[None]], axis=0).astype(jnp.float32)
    sample_total = voxel_bins.shape[0]
    slab_count = slab_order.shape[1]
    tile_count = slab_order.shape[0]
    row_count = voxel_bins.shape[1]
    col_count = voxel_bins.shape[2]
    extinct_rate = 3.0 / sample_total
    slabs = voxel_bins.reshape(slab_count, sample_total // slab_count, row_count, col_count)

    def march(slab):
        def advance(carried, layer):
            passed, color_sum = carried
            values = jnp.take(table, layer, axis=1)
            density = values[3]
            weight = (1.0 - jnp.exp(-extinct_rate * density)) * jnp.exp(-extinct_rate * passed)
            return (passed + density, color_sum + weight[None] * values[:3]), None

        start = (jnp.zeros((row_count, col_count), jnp.float32), jnp.zeros((3, row_count, col_count), jnp.float32))
        (passed, color_sum), ignored = lax.scan(advance, start, slab)
        final_alpha = 1.0 - jnp.exp(-extinct_rate * passed)
        return jnp.concatenate([color_sum, final_alpha[None]], axis=0)

    partials = lax.map(march, slabs)
    pieces = partials.reshape(slab_count, 4, row_count, tile_count, col_count // tile_count)
    acc_color = jnp.zeros((3, row_count, tile_count, col_count // tile_count), jnp.float32)
    acc_alpha = jnp.zeros((row_count, tile_count, col_count // tile_count), jnp.float32)
    for place in range(slab_count):
        select = (slab_order == place).astype(jnp.float32)
        picked = jnp.einsum("ti,icrtw->crtw", select, pieces, precision=lax.Precision.HIGHEST)
        acc_color = acc_color + (1.0 - acc_alpha)[None] * picked[:3]
        acc_alpha = acc_alpha + (1.0 - acc_alpha) * picked[3]
    merged = jnp.concatenate([acc_color, acc_alpha[None]], axis=0)
    return merged.reshape(4, row_count, col_count)
```

```python
import functools

import jax
import jax.numpy as jnp
from jax import lax
from jax.experimental import pallas as pl
from jax.experimental.pallas import tpu as pltpu
from jax.sharding import PartitionSpec as P

extinction = 3.0
lanes = 128
MESH = pl.DeviceIdType.MESH


def flip(index, mask):
    result = index
    bit = 1
    while bit <= mask:
        if mask & bit:
            result = result + bit * (1 - 2 * lax.rem(lax.div(index, bit), 2))
        bit *= 2
    return result


def kernel(
    sizes,
    order_ref,
    bins_hbm,
    colors_ref,
    opacity_ref,
    out_ref,
    bins,
    sent,
    own,
    arrived,
    merged,
    bins_sem,
    send_sem,
    recv_sem,
    row_send_sem,
    row_recv_sem,
):
    depth_count, tile_count, samples, unit_rows, units, owners, rows_each, cols, rate = sizes
    depth = lax.axis_index("depth")
    tile = lax.axis_index("screen")
    own_unit = lax.div(tile, owners)
    own_place = lax.rem(tile, owners)
    steps = list(range(units - 1, -1, -1))
    peers = [depth_count - 1] + list(range(1, depth_count - 1)) + [0]

    barrier = pltpu.get_barrier_semaphore()
    for mask in range(1, depth_count):
        pl.semaphore_signal(
            barrier, inc=1, device_id=(flip(depth, mask), tile), device_id_type=MESH
        )
    for mask in range(1, tile_count):
        pl.semaphore_signal(
            barrier, inc=1, device_id=(depth, flip(tile, mask)), device_id_type=MESH
        )

    def fetch(step, mask):
        row = (flip(depth, mask) * units + flip(own_unit, step)) * unit_rows
        row = pl.multiple_of(row, unit_rows)
        return pltpu.make_async_copy(
            bins_hbm.at[:, pl.ds(row, unit_rows), :],
            bins.at[step, mask],
            bins_sem.at[step, mask],
        )

    for step in steps:
        for mask in peers:
            if mask:
                fetch(step, mask).start()
    for step in steps:
        fetch(step, 0).start()

    density = opacity_ref[...].astype(jnp.float32)
    weight = 1.0 - jnp.exp(-rate * density)
    shades = weight * colors_ref[...].astype(jnp.float32)
    table = [shades[c : c + 1] for c in range(3)] + [weight]
    bin_count = weight.shape[1]
    parts = [
        [jnp.broadcast_to(row[:, at : at + lanes], (8, lanes)) for at in range(0, bin_count, lanes)]
        for row in table
    ]

    def march(step, mask, target):
        for row in range(0, unit_rows, 8):
            for col in range(0, cols, lanes):
                clear = None
                total = None
                for j in range(samples):
                    index = bins[step, mask, j, row : row + 8, col : col + lanes]
                    low = lax.rem(index, lanes) if lanes & (lanes - 1) else index & (lanes - 1)
                    values = []
                    for part in parts:
                        value = jnp.take_along_axis(part[0], low, axis=1, mode="promise_in_bounds")
                        for n in range(1, len(part)):
                            other = jnp.take_along_axis(
                                part[n], low, axis=1, mode="promise_in_bounds"
                            )
                            value = jnp.where(index >= n * lanes, other, value)
                        values.append(value)
                    if total is None:
                        total = values
                        clear = 1.0 - values[3]
                    else:
                        seen = clear * values[3]
                        total = [t + clear * v for t, v in zip(total[:3], values[:3])] + [
                            total[3] + seen
                        ]
                        clear = clear - seen
                for c in range(4):
                    target[c, row : row + 8, col : col + lanes] = total[c]

    def send(step, mask):
        return pltpu.make_async_remote_copy(
            src_ref=sent.at[step, mask - 1],
            dst_ref=arrived.at[step, mask - 1],
            send_sem=send_sem.at[step, mask - 1],
            recv_sem=recv_sem.at[step, mask - 1],
            device_id=(flip(depth, mask), tile),
            device_id_type=MESH,
        )

    def send_row(step, low):
        mask = step * owners + low
        place = flip(own_place, low)
        there = pl.ds(pl.multiple_of(tile * cols, lanes), cols)
        return pltpu.make_async_remote_copy(
            src_ref=merged.at[step, place],
            dst_ref=out_ref.at[:, :, there],
            send_sem=row_send_sem.at[mask],
            recv_sem=row_recv_sem.at[mask],
            device_id=(depth, flip(tile, mask)),
            device_id_type=MESH,
        )

    def take_row(mask):
        here = pl.ds(pl.multiple_of(flip(tile, mask) * cols, lanes), cols)
        return pltpu.make_async_remote_copy(
            src_ref=merged.at[0, 0],
            dst_ref=out_ref.at[:, :, here],
            send_sem=row_send_sem.at[mask],
            recv_sem=row_recv_sem.at[mask],
            device_id=(depth, flip(tile, mask)),
            device_id_type=MESH,
        )

    for step in steps:
        for mask in peers:
            if mask:
                fetch(step, mask).wait()
                march(step, mask, sent.at[step, mask - 1])
        if step == steps[0]:
            pl.semaphore_wait(barrier, depth_count + tile_count - 2)
        for mask in peers:
            if mask:
                send(step, mask).start()
    for step in steps:
        fetch(step, 0).wait()
        march(step, 0, own.at[step])

    place_of = [order_ref[tile, flip(depth, mask)] for mask in range(depth_count)]
    ahead = [
        [jnp.where(place_of[j] < place_of[i], 1.0, 0.0) for j in range(depth_count)]
        for i in range(depth_count)
    ]

    for step in steps:
        for mask in peers:
            if mask:
                send(step, mask).wait_recv()
        for row in range(0, unit_rows, 8):
            for col in range(0, cols, lanes):
                window = (slice(row, row + 8), slice(col, col + lanes))
                pieces = [
                    own[(step, slice(None)) + window]
                    if mask == 0
                    else arrived[(step, mask - 1, slice(None)) + window]
                    for mask in range(depth_count)
                ]
                total = None
                for i in range(depth_count):
                    front = None
                    for j in range(depth_count):
                        if j != i:
                            passed = 1.0 - ahead[i][j] * pieces[j][3]
                            front = passed if front is None else front * passed
                    lit = [pieces[i][c] if front is None else pieces[i][c] * front for c in range(4)]
                    total = lit if total is None else [t + v for t, v in zip(total, lit)]
                for c in range(4):
                    if owners == 1:
                        merged[step, 0, c, row : row + 8, col : col + lanes] = total[c]
                    else:
                        for place in range(owners):
                            merged[step, place, c, :, col : col + lanes] = total[c][
                                place * rows_each : (place + 1) * rows_each
                            ]
        for low in range(owners - 1, -1, -1):
            if step * owners + low:
                send_row(step, low).start()
            else:
                here = pl.ds(pl.multiple_of(tile * cols, lanes), cols)
                out_ref[:, :, here] = merged[step, own_place]

    for mask in range(tile_count - 1, 0, -1):
        take_row(mask).wait_recv()
    for step in steps:
        for mask in range(1, depth_count):
            send(step, mask).wait_send()
    for mask in range(1, tile_count):
        send_row(mask // owners, mask % owners).wait_send()


def local(voxel_bins, colors, opacity, slab_order):
    depth_count = lax.axis_size("depth")
    tile_count = lax.axis_size("screen")
    samples, row_count, cols = voxel_bins.shape
    rows_each = row_count // (depth_count * tile_count)
    unit_rows = max(8, rows_each)
    owners = unit_rows // rows_each
    units = tile_count // owners
    rate = extinction / (samples * depth_count)
    sizes = (depth_count, tile_count, samples, unit_rows, units, owners, rows_each, cols, rate)
    others = depth_count - 1
    vmem = pl.BlockSpec(memory_space=pltpu.VMEM)
    return pl.pallas_call(
        functools.partial(kernel, sizes),
        out_shape=jax.ShapeDtypeStruct((4, rows_each, cols * tile_count), jnp.float32),
        in_specs=[
            pl.BlockSpec(memory_space=pltpu.SMEM),
            pl.BlockSpec(memory_space=pl.ANY),
            vmem,
            vmem,
        ],
        out_specs=vmem,
        scratch_shapes=[
            pltpu.VMEM((units, depth_count, samples, unit_rows, cols), jnp.int32),
            pltpu.VMEM((units, others, 4, unit_rows, cols), jnp.float32),
            pltpu.VMEM((units, 4, unit_rows, cols), jnp.float32),
            pltpu.VMEM((units, others, 4, unit_rows, cols), jnp.float32),
            pltpu.VMEM((units, owners, 4, rows_each, cols), jnp.float32),
            pltpu.SemaphoreType.DMA((units, depth_count)),
            pltpu.SemaphoreType.DMA((units, others)),
            pltpu.SemaphoreType.DMA((units, others)),
            pltpu.SemaphoreType.DMA((tile_count,)),
            pltpu.SemaphoreType.DMA((tile_count,)),
        ],
        compiler_params=pltpu.CompilerParams(collective_id=0, has_side_effects=True),
    )(slab_order, voxel_bins, colors, opacity[None])


def solution(mesh):
    placed = (P("depth", None, "screen"), P(), P(), P())
    return jax.shard_map(
        local,
        mesh=mesh,
        in_specs=placed,
        out_specs=P(None, ("depth", "screen"), None),
        check_vma=False,
    )
```

```python
import functools

import jax
import jax.numpy as jnp
from jax import lax
from jax.experimental import pallas as pl
from jax.experimental.pallas import tpu as pltpu
from jax.sharding import PartitionSpec as P

extinction = 3.0
lanes = 128
MESH = pl.DeviceIdType.MESH


def flip(index, mask):
    result = index
    bit = 1
    while bit <= mask:
        if mask & bit:
            result = result + bit * (1 - 2 * lax.rem(lax.div(index, bit), 2))
        bit *= 2
    return result


def kernel(
    sizes,
    order_ref,
    bins_hbm,
    colors_ref,
    opacity_ref,
    out_ref,
    bins,
    sent,
    own,
    arrived,
    merged,
    bins_sem,
    send_sem,
    recv_sem,
    row_send_sem,
    row_recv_sem,
):
    depth_count, tile_count, samples, unit_rows, units, owners, rows_each, cols, rate = sizes
    depth = lax.axis_index("depth")
    tile = lax.axis_index("screen")
    own_unit = lax.div(tile, owners)
    own_place = lax.rem(tile, owners)
    steps = list(range(units - 1, -1, -1))
    peers = [depth_count - 1] + list(range(1, depth_count - 1)) + [0]

    barrier = pltpu.get_barrier_semaphore()
    for mask in range(1, depth_count):
        pl.semaphore_signal(
            barrier, inc=1, device_id=(flip(depth, mask), tile), device_id_type=MESH
        )
    for mask in range(1, tile_count):
        pl.semaphore_signal(
            barrier, inc=1, device_id=(depth, flip(tile, mask)), device_id_type=MESH
        )

    def fetch(step, mask):
        row = (flip(depth, mask) * units + flip(own_unit, step)) * unit_rows
        row = pl.multiple_of(row, unit_rows)
        return pltpu.make_async_copy(
            bins_hbm.at[:, pl.ds(row, unit_rows), :],
            bins.at[step, mask],
            bins_sem.at[step, mask],
        )

    for step in steps:
        for mask in peers:
            if mask:
                fetch(step, mask).start()
    for step in steps:
        fetch(step, 0).start()

    density = opacity_ref[...].astype(jnp.float32).reshape(1, -1)
    weight = 1.0 - jnp.exp(-rate * density)
    shades = weight * colors_ref[...].astype(jnp.float32)
    table = [shades[c : c + 1] for c in range(3)] + [weight]
    bin_count = weight.shape[1]
    parts = [
        [jnp.broadcast_to(row[:, at : at + lanes], (8, lanes)) for at in range(0, bin_count, lanes)]
        for row in table
    ]

    def march(step, mask, target):
        for row in range(0, unit_rows, 8):
            for col in range(0, cols, lanes):
                clear = None
                total = None
                for j in range(samples):
                    index = bins[step, mask, j, row : row + 8, col : col + lanes]
                    low = lax.rem(index, lanes) if lanes & (lanes - 1) else index & (lanes - 1)
                    values = []
                    for part in parts:
                        value = jnp.take_along_axis(part[0], low, axis=1, mode="promise_in_bounds")
                        for n in range(1, len(part)):
                            other = jnp.take_along_axis(
                                part[n], low, axis=1, mode="promise_in_bounds"
                            )
                            value = jnp.where(index >= n * lanes, other, value)
                        values.append(value)
                    if total is None:
                        total = values
                        clear = 1.0 - values[3]
                    else:
                        seen = clear * values[3]
                        total = [t + clear * v for t, v in zip(total[:3], values[:3])] + [
                            total[3] + seen
                        ]
                        clear = clear - seen
                for c in range(4):
                    target[c, row : row + 8, col : col + lanes] = total[c]

    def send(step, mask):
        return pltpu.make_async_remote_copy(
            src_ref=sent.at[step, mask - 1],
            dst_ref=arrived.at[step, mask - 1],
            send_sem=send_sem.at[step, mask - 1],
            recv_sem=recv_sem.at[step, mask - 1],
            device_id=(flip(depth, mask), tile),
            device_id_type=MESH,
        )

    def send_row(step, low):
        mask = step * owners + low
        place = flip(own_place, low)
        there = pl.ds(pl.multiple_of(tile * cols, lanes), cols)
        return pltpu.make_async_remote_copy(
            src_ref=merged.at[step, place],
            dst_ref=out_ref.at[:, :, there],
            send_sem=row_send_sem.at[mask],
            recv_sem=row_recv_sem.at[mask],
            device_id=(depth, flip(tile, mask)),
            device_id_type=MESH,
        )

    def take_row(mask):
        here = pl.ds(pl.multiple_of(flip(tile, mask) * cols, lanes), cols)
        return pltpu.make_async_remote_copy(
            src_ref=merged.at[0, 0],
            dst_ref=out_ref.at[:, :, here],
            send_sem=row_send_sem.at[mask],
            recv_sem=row_recv_sem.at[mask],
            device_id=(depth, flip(tile, mask)),
            device_id_type=MESH,
        )

    for step in steps:
        for mask in peers:
            if mask:
                fetch(step, mask).wait()
                march(step, mask, sent.at[step, mask - 1])
        if step == steps[0]:
            pl.semaphore_wait(barrier, depth_count + tile_count - 2)
        for mask in peers:
            if mask:
                send(step, mask).start()
    for step in steps:
        fetch(step, 0).wait()
        march(step, 0, own.at[step])

    place_of = [order_ref[flip(depth, mask), tile] for mask in range(depth_count)]
    ahead = [
        [jnp.where(place_of[j] < place_of[i], 1.0, 0.0) for j in range(depth_count)]
        for i in range(depth_count)
    ]

    for step in steps:
        for mask in peers:
            if mask:
                send(step, mask).wait_recv()
        for row in range(0, unit_rows, 8):
            for col in range(0, cols, lanes):
                window = (slice(row, row + 8), slice(col, col + lanes))
                pieces = [
                    own[(step, slice(None)) + window]
                    if mask == 0
                    else arrived[(step, mask - 1, slice(None)) + window]
                    for mask in range(depth_count)
                ]
                total = None
                for i in range(depth_count):
                    front = None
                    for j in range(depth_count):
                        if j != i:
                            passed = 1.0 - ahead[i][j] * pieces[j][3]
                            front = passed if front is None else front * passed
                    lit = [pieces[i][c] if front is None else pieces[i][c] * front for c in range(4)]
                    total = lit if total is None else [t + v for t, v in zip(total, lit)]
                for c in range(4):
                    if owners == 1:
                        merged[step, 0, c, row : row + 8, col : col + lanes] = total[c]
                    else:
                        for place in range(owners):
                            merged[step, place, c, :, col : col + lanes] = total[c][
                                place * rows_each : (place + 1) * rows_each
                            ]
        for low in range(owners - 1, -1, -1):
            if step * owners + low:
                send_row(step, low).start()
            else:
                here = pl.ds(pl.multiple_of(tile * cols, lanes), cols)
                out_ref[:, :, here] = merged[step, own_place]

    for mask in range(tile_count - 1, 0, -1):
        take_row(mask).wait_recv()
    for step in steps:
        for mask in range(1, depth_count):
            send(step, mask).wait_send()
    for mask in range(1, tile_count):
        send_row(mask // owners, mask % owners).wait_send()


def local(voxel_bins, colors, opacity, slab_order):
    depth_count = lax.axis_size("depth")
    tile_count = lax.axis_size("screen")
    samples, row_count, cols = voxel_bins.shape
    rows_each = row_count // (depth_count * tile_count)
    unit_rows = max(8, rows_each)
    owners = unit_rows // rows_each
    units = tile_count // owners
    rate = extinction / (samples * depth_count)
    sizes = (depth_count, tile_count, samples, unit_rows, units, owners, rows_each, cols, rate)
    others = depth_count - 1
    vmem = pl.BlockSpec(memory_space=pltpu.VMEM)
    return pl.pallas_call(
        functools.partial(kernel, sizes),
        out_shape=pltpu.VMEM((4, rows_each, cols * tile_count), jnp.float32),
        in_specs=[
            pl.BlockSpec(memory_space=pltpu.SMEM),
            pl.BlockSpec(memory_space=pl.ANY),
            vmem,
            vmem,
        ],
        out_specs=vmem,
        scratch_shapes=[
            pltpu.VMEM((units, depth_count, samples, unit_rows, cols), jnp.int32),
            pltpu.VMEM((units, others, 4, unit_rows, cols), jnp.float32),
            pltpu.VMEM((units, 4, unit_rows, cols), jnp.float32),
            pltpu.VMEM((units, others, 4, unit_rows, cols), jnp.float32),
            pltpu.VMEM((units, owners, 4, rows_each, cols), jnp.float32),
            pltpu.SemaphoreType.DMA((units, depth_count)),
            pltpu.SemaphoreType.DMA((units, others)),
            pltpu.SemaphoreType.DMA((units, others)),
            pltpu.SemaphoreType.DMA((tile_count,)),
            pltpu.SemaphoreType.DMA((tile_count,)),
        ],
        compiler_params=pltpu.CompilerParams(collective_id=0, has_side_effects=True),
    )(slab_order.T, voxel_bins, colors, opacity)


def solution(mesh):
    placed = (P("depth", None, "screen"), P(), P(), P())
    return jax.shard_map(
        local,
        mesh=mesh,
        in_specs=placed,
        out_specs=P(None, ("depth", "screen"), None),
        check_vma=False,
    )
```

```python
import functools

import jax
import jax.numpy as jnp
from jax import lax
from jax.experimental import pallas as pl
from jax.experimental.pallas import tpu as pltpu
from jax.sharding import PartitionSpec as P

extinction = 3.0
lanes = 128
MESH = pl.DeviceIdType.MESH


def flip(index, mask, count):
    result = index
    bit = 1
    while bit < count:
        if isinstance(mask, int):
            if mask & bit:
                result = result + bit * (1 - 2 * lax.rem(lax.div(index, bit), 2))
        else:
            mine = lax.rem(lax.div(index, bit), 2)
            other = lax.rem(lax.div(mask, bit), 2)
            result = result + bit * other * (1 - 2 * mine)
        bit *= 2
    return result


def kernel(
    sizes,
    order_ref,
    bins_hbm,
    colors_ref,
    opacity_ref,
    out_ref,
    bins,
    sent,
    own,
    arrived,
    merged,
    bins_sem,
    send_sem,
    recv_sem,
    row_send_sem,
    row_recv_sem,
):
    depth_count, tile_count, samples, unit_rows, units, owners, rows_each, cols, rate = sizes
    depth = lax.axis_index("depth")
    tile = lax.axis_index("screen")
    own_unit = lax.div(tile, owners)
    own_place = lax.rem(tile, owners)
    steps = list(range(units - 1, -1, -1))
    peers = [depth_count - 1] + list(range(1, depth_count - 1)) + [0]

    barrier = pltpu.get_barrier_semaphore()
    for mask in range(1, depth_count):
        pl.semaphore_signal(
            barrier, inc=1, device_id=(flip(depth, mask, depth_count), tile), device_id_type=MESH
        )
    for mask in range(1, tile_count):
        pl.semaphore_signal(
            barrier, inc=1, device_id=(depth, flip(tile, mask, tile_count)), device_id_type=MESH
        )

    def fetch(step, mask):
        row = (flip(depth, mask, depth_count) * units + flip(own_unit, step, units)) * unit_rows
        row = pl.multiple_of(row, unit_rows)
        return pltpu.make_async_copy(
            bins_hbm.at[:, pl.ds(row, unit_rows), :],
            bins.at[step, mask],
            bins_sem.at[step, mask],
        )

    for step in steps:
        for mask in peers:
            if mask:
                fetch(step, mask).start()
    for step in steps:
        fetch(step, 0).start()

    density = opacity_ref[...].astype(jnp.float32).reshape(1, -1)
    weight = 1.0 - jnp.exp(-rate * density)
    shades = weight * colors_ref[...].astype(jnp.float32)
    table = [shades[c : c + 1] for c in range(3)] + [weight]
    bin_count = weight.shape[1]
    parts = [
        [jnp.broadcast_to(row[:, at : at + lanes], (8, lanes)) for at in range(0, bin_count, lanes)]
        for row in table
    ]

    def march(step, mask, target):
        for row in range(0, unit_rows, 8):
            for col in range(0, cols, lanes):
                clear = None
                total = None
                for j in range(samples):
                    index = bins[step, mask, j, row : row + 8, col : col + lanes]
                    low = lax.rem(index, lanes) if lanes & (lanes - 1) else index & (lanes - 1)
                    values = []
                    for part in parts:
                        value = jnp.take_along_axis(part[0], low, axis=1, mode="promise_in_bounds")
                        for n in range(1, len(part)):
                            other = jnp.take_along_axis(
                                part[n], low, axis=1, mode="promise_in_bounds"
                            )
                            value = jnp.where(index >= n * lanes, other, value)
                        values.append(value)
                    if total is None:
                        total = values
                        clear = 1.0 - values[3]
                    else:
                        seen = clear * values[3]
                        total = [t + clear * v for t, v in zip(total[:3], values[:3])] + [
                            total[3] + seen
                        ]
                        clear = clear - seen
                for c in range(4):
                    target[c, row : row + 8, col : col + lanes] = total[c]

    def send(step, mask):
        return pltpu.make_async_remote_copy(
            src_ref=sent.at[step, mask - 1],
            dst_ref=arrived.at[step, mask - 1],
            send_sem=send_sem.at[step, mask - 1],
            recv_sem=recv_sem.at[step, mask - 1],
            device_id=(flip(depth, mask, depth_count), tile),
            device_id_type=MESH,
        )

    def send_row(step, low):
        mask = step * owners + low
        place = flip(own_place, low, owners)
        there = pl.ds(pl.multiple_of(tile * cols, lanes), cols)
        return pltpu.make_async_remote_copy(
            src_ref=merged.at[step, place],
            dst_ref=out_ref.at[:, :, there],
            send_sem=row_send_sem.at[mask],
            recv_sem=row_recv_sem.at[mask],
            device_id=(depth, flip(tile, mask, tile_count)),
            device_id_type=MESH,
        )

    def take_row(mask):
        here = pl.ds(pl.multiple_of(flip(tile, mask, tile_count) * cols, lanes), cols)
        return pltpu.make_async_remote_copy(
            src_ref=merged.at[0, 0],
            dst_ref=out_ref.at[:, :, here],
            send_sem=row_send_sem.at[mask],
            recv_sem=row_recv_sem.at[mask],
            device_id=(depth, flip(tile, mask, tile_count)),
            device_id_type=MESH,
        )

    def feed(n, carry):
        step = units - 1 - n
        for mask in peers:
            if mask:
                fetch(step, mask).wait()
                march(step, mask, sent.at[step, mask - 1])

        @pl.when(n == 0)
        def _():
            pl.semaphore_wait(barrier, depth_count + tile_count - 2)

        for mask in peers:
            if mask:
                send(step, mask).start()
        return carry

    lax.fori_loop(0, units, feed, 0)

    def keep(n, carry):
        step = units - 1 - n
        fetch(step, 0).wait()
        march(step, 0, own.at[step])
        return carry

    lax.fori_loop(0, units, keep, 0)

    place_of = [order_ref[flip(depth, mask, depth_count), tile] for mask in range(depth_count)]
    ahead = [
        [jnp.where(place_of[j] < place_of[i], 1.0, 0.0) for j in range(depth_count)]
        for i in range(depth_count)
    ]

    def blend(n, carry):
        step = units - 1 - n
        for mask in peers:
            if mask:
                send(step, mask).wait_recv()
        for row in range(0, unit_rows, 8):
            for col in range(0, cols, lanes):
                window = (slice(row, row + 8), slice(col, col + lanes))
                pieces = [
                    own[(step, slice(None)) + window]
                    if mask == 0
                    else arrived[(step, mask - 1, slice(None)) + window]
                    for mask in range(depth_count)
                ]
                total = None
                for i in range(depth_count):
                    front = None
                    for j in range(depth_count):
                        if j != i:
                            passed = 1.0 - ahead[i][j] * pieces[j][3]
                            front = passed if front is None else front * passed
                    lit = [pieces[i][c] if front is None else pieces[i][c] * front for c in range(4)]
                    total = lit if total is None else [t + v for t, v in zip(total, lit)]
                for c in range(4):
                    if owners == 1:
                        merged[step, 0, c, row : row + 8, col : col + lanes] = total[c]
                    else:
                        for place in range(owners):
                            merged[step, place, c, :, col : col + lanes] = total[c][
                                place * rows_each : (place + 1) * rows_each
                            ]
        for low in range(owners - 1, 0, -1):
            send_row(step, low).start()

        @pl.when(step > 0)
        def _():
            send_row(step, 0).start()

        return carry

    lax.fori_loop(0, units, blend, 0)
    here = pl.ds(pl.multiple_of(tile * cols, lanes), cols)
    out_ref[:, :, here] = merged[0, own_place]

    for mask in range(tile_count - 1, 0, -1):
        take_row(mask).wait_recv()
    for step in steps:
        for mask in range(1, depth_count):
            send(step, mask).wait_send()
    for mask in range(1, tile_count):
        send_row(mask // owners, mask % owners).wait_send()


def local(voxel_bins, colors, opacity, slab_order):
    depth_count = lax.axis_size("depth")
    tile_count = lax.axis_size("screen")
    samples, row_count, cols = voxel_bins.shape
    rows_each = row_count // (depth_count * tile_count)
    unit_rows = max(8, rows_each)
    owners = unit_rows // rows_each
    units = tile_count // owners
    rate = extinction / (samples * depth_count)
    sizes = (depth_count, tile_count, samples, unit_rows, units, owners, rows_each, cols, rate)
    others = depth_count - 1
    vmem = pl.BlockSpec(memory_space=pltpu.VMEM)
    return pl.pallas_call(
        functools.partial(kernel, sizes),
        out_shape=pltpu.VMEM((4, rows_each, cols * tile_count), jnp.float32),
        in_specs=[
            pl.BlockSpec(memory_space=pltpu.SMEM),
            pl.BlockSpec(memory_space=pl.ANY),
            vmem,
            vmem,
        ],
        out_specs=vmem,
        scratch_shapes=[
            pltpu.VMEM((units, depth_count, samples, unit_rows, cols), jnp.int32),
            pltpu.VMEM((units, others, 4, unit_rows, cols), jnp.float32),
            pltpu.VMEM((units, 4, unit_rows, cols), jnp.float32),
            pltpu.VMEM((units, others, 4, unit_rows, cols), jnp.float32),
            pltpu.VMEM((units, owners, 4, rows_each, cols), jnp.float32),
            pltpu.SemaphoreType.DMA((units, depth_count)),
            pltpu.SemaphoreType.DMA((units, others)),
            pltpu.SemaphoreType.DMA((units, others)),
            pltpu.SemaphoreType.DMA((tile_count,)),
            pltpu.SemaphoreType.DMA((tile_count,)),
        ],
        compiler_params=pltpu.CompilerParams(collective_id=0, has_side_effects=True),
    )(slab_order.T, voxel_bins, colors, opacity)


def solution(mesh):
    placed = (P("depth", None, "screen"), P(), P(), P())
    return jax.shard_map(
        local,
        mesh=mesh,
        in_specs=placed,
        out_specs=P(None, ("depth", "screen"), None),
        check_vma=False,
    )
```

```python
import functools

import jax
import jax.numpy as jnp
from jax import lax
from jax.experimental import pallas as pl
from jax.experimental.pallas import tpu as pltpu
from jax.sharding import PartitionSpec as P

extinction = 3.0
lanes = 128
MESH = pl.DeviceIdType.MESH


def flip(index, mask, count):
    result = index
    bit = 1
    while bit < count:
        if isinstance(mask, int):
            if mask & bit:
                result = result + bit * (1 - 2 * lax.rem(lax.div(index, bit), 2))
        else:
            mine = lax.rem(lax.div(index, bit), 2)
            other = lax.rem(lax.div(mask, bit), 2)
            result = result + bit * other * (1 - 2 * mine)
        bit *= 2
    return result


def kernel(
    sizes,
    order_ref,
    bins_hbm,
    colors_ref,
    opacity_ref,
    out_ref,
    bins,
    sent,
    own,
    arrived,
    merged,
    bins_sem,
    send_sem,
    recv_sem,
    row_send_sem,
    row_recv_sem,
    ready_sem,
    go_sem,
):
    depth_count, tile_count, samples, unit_rows, units, owners, rows_each, cols, rate = sizes
    depth = lax.axis_index("depth")
    tile = lax.axis_index("screen")
    own_unit = lax.div(tile, owners)
    own_place = lax.rem(tile, owners)
    steps = list(range(units - 1, -1, -1))
    peers = [depth_count - 1] + list(range(1, depth_count - 1)) + [0]

    barrier = pltpu.get_barrier_semaphore()
    hub = depth == 0
    for mask in range(1, depth_count):
        peer = flip(depth, mask, depth_count)

        @pl.when(peer != 0)
        def _():
            pl.semaphore_signal(barrier, inc=1, device_id=(peer, tile), device_id_type=MESH)

    def meet_depth():
        @pl.when(jnp.logical_not(hub))
        def _():
            pl.semaphore_wait(barrier, depth_count - 1)
            pl.semaphore_signal(ready_sem, inc=1, device_id=(0, tile), device_id_type=MESH)

        @pl.when(hub)
        def _():
            pl.semaphore_wait(ready_sem, depth_count - 1)
            for mask in range(1, tile_count):
                pl.semaphore_signal(
                    barrier,
                    inc=1,
                    device_id=(0, flip(tile, mask, tile_count)),
                    device_id_type=MESH,
                )

    def meet_tiles():
        @pl.when(hub)
        def _():
            pl.semaphore_wait(barrier, tile_count - 1)
            for mask in range(1, depth_count):
                pl.semaphore_signal(go_sem, inc=1, device_id=(mask, tile), device_id_type=MESH)

        @pl.when(jnp.logical_not(hub))
        def _():
            pl.semaphore_wait(go_sem, 1)

    def fetch(step, mask):
        row = (flip(depth, mask, depth_count) * units + flip(own_unit, step, units)) * unit_rows
        row = pl.multiple_of(row, unit_rows)
        return pltpu.make_async_copy(
            bins_hbm.at[:, pl.ds(row, unit_rows), :],
            bins.at[step, mask],
            bins_sem.at[step, mask],
        )

    for step in steps:
        for mask in peers:
            if mask:
                fetch(step, mask).start()
    for step in steps:
        fetch(step, 0).start()

    density = opacity_ref[...].astype(jnp.float32).reshape(1, -1)
    weight = 1.0 - jnp.exp(-rate * density)
    shades = weight * colors_ref[...].astype(jnp.float32)
    table = [shades[c : c + 1] for c in range(3)] + [weight]
    bin_count = weight.shape[1]
    parts = [
        [jnp.broadcast_to(row[:, at : at + lanes], (8, lanes)) for at in range(0, bin_count, lanes)]
        for row in table
    ]

    def march(step, mask, target):
        for row in range(0, unit_rows, 8):
            for col in range(0, cols, lanes):
                clear = None
                total = None
                for j in range(samples):
                    index = bins[step, mask, j, row : row + 8, col : col + lanes]
                    low = lax.rem(index, lanes) if lanes & (lanes - 1) else index & (lanes - 1)
                    values = []
                    for part in parts:
                        value = jnp.take_along_axis(part[0], low, axis=1, mode="promise_in_bounds")
                        for n in range(1, len(part)):
                            other = jnp.take_along_axis(
                                part[n], low, axis=1, mode="promise_in_bounds"
                            )
                            value = jnp.where(index >= n * lanes, other, value)
                        values.append(value)
                    if total is None:
                        total = values
                        clear = 1.0 - values[3]
                    else:
                        seen = clear * values[3]
                        total = [t + clear * v for t, v in zip(total[:3], values[:3])] + [
                            total[3] + seen
                        ]
                        clear = clear - seen
                for c in range(4):
                    target[c, row : row + 8, col : col + lanes] = total[c]

    def send(step, mask):
        return pltpu.make_async_remote_copy(
            src_ref=sent.at[step, mask - 1],
            dst_ref=arrived.at[step, mask - 1],
            send_sem=send_sem.at[step, mask - 1],
            recv_sem=recv_sem.at[step, mask - 1],
            device_id=(flip(depth, mask, depth_count), tile),
            device_id_type=MESH,
        )

    def send_row(step, low):
        mask = step * owners + low
        place = flip(own_place, low, owners)
        there = pl.ds(pl.multiple_of(tile * cols, lanes), cols)
        return pltpu.make_async_remote_copy(
            src_ref=merged.at[step, place],
            dst_ref=out_ref.at[:, :, there],
            send_sem=row_send_sem.at[mask],
            recv_sem=row_recv_sem.at[mask],
            device_id=(depth, flip(tile, mask, tile_count)),
            device_id_type=MESH,
        )

    def take_row(mask):
        here = pl.ds(pl.multiple_of(flip(tile, mask, tile_count) * cols, lanes), cols)
        return pltpu.make_async_remote_copy(
            src_ref=merged.at[0, 0],
            dst_ref=out_ref.at[:, :, here],
            send_sem=row_send_sem.at[mask],
            recv_sem=row_recv_sem.at[mask],
            device_id=(depth, flip(tile, mask, tile_count)),
            device_id_type=MESH,
        )

    def feed(n, carry):
        step = units - 1 - n
        for mask in peers:
            if mask:
                fetch(step, mask).wait()
                march(step, mask, sent.at[step, mask - 1])

        @pl.when(n == 0)
        def _():
            meet_depth()

        for mask in peers:
            if mask:
                send(step, mask).start()
        return carry

    lax.fori_loop(0, units, feed, 0)

    def keep(n, carry):
        step = units - 1 - n
        fetch(step, 0).wait()
        march(step, 0, own.at[step])
        return carry

    lax.fori_loop(0, units, keep, 0)
    meet_tiles()

    place_of = [order_ref[flip(depth, mask, depth_count), tile] for mask in range(depth_count)]
    ahead = [
        [jnp.where(place_of[j] < place_of[i], 1.0, 0.0) for j in range(depth_count)]
        for i in range(depth_count)
    ]

    def blend(n, carry):
        step = units - 1 - n
        for mask in peers:
            if mask:
                send(step, mask).wait_recv()
        for row in range(0, unit_rows, 8):
            for col in range(0, cols, lanes):
                window = (slice(row, row + 8), slice(col, col + lanes))
                pieces = [
                    own[(step, slice(None)) + window]
                    if mask == 0
                    else arrived[(step, mask - 1, slice(None)) + window]
                    for mask in range(depth_count)
                ]
                total = None
                for i in range(depth_count):
                    front = None
                    for j in range(depth_count):
                        if j != i:
                            passed = 1.0 - ahead[i][j] * pieces[j][3]
                            front = passed if front is None else front * passed
                    lit = [pieces[i][c] if front is None else pieces[i][c] * front for c in range(4)]
                    total = lit if total is None else [t + v for t, v in zip(total, lit)]
                for c in range(4):
                    if owners == 1:
                        merged[step, 0, c, row : row + 8, col : col + lanes] = total[c]
                    else:
                        for place in range(owners):
                            merged[step, place, c, :, col : col + lanes] = total[c][
                                place * rows_each : (place + 1) * rows_each
                            ]
        for low in range(owners - 1, 0, -1):
            send_row(step, low).start()

        @pl.when(step > 0)
        def _():
            send_row(step, 0).start()

        return carry

    lax.fori_loop(0, units, blend, 0)
    here = pl.ds(pl.multiple_of(tile * cols, lanes), cols)
    out_ref[:, :, here] = merged[0, own_place]

    for mask in range(tile_count - 1, 0, -1):
        take_row(mask).wait_recv()
    for step in steps:
        for mask in range(1, depth_count):
            send(step, mask).wait_send()
    for mask in range(1, tile_count):
        send_row(mask // owners, mask % owners).wait_send()


def local(voxel_bins, colors, opacity, slab_order):
    depth_count = lax.axis_size("depth")
    tile_count = lax.axis_size("screen")
    samples, row_count, cols = voxel_bins.shape
    rows_each = row_count // (depth_count * tile_count)
    unit_rows = max(8, rows_each)
    owners = unit_rows // rows_each
    units = tile_count // owners
    rate = extinction / (samples * depth_count)
    sizes = (depth_count, tile_count, samples, unit_rows, units, owners, rows_each, cols, rate)
    others = depth_count - 1
    vmem = pl.BlockSpec(memory_space=pltpu.VMEM)
    return pl.pallas_call(
        functools.partial(kernel, sizes),
        out_shape=pltpu.VMEM((4, rows_each, cols * tile_count), jnp.float32),
        in_specs=[
            pl.BlockSpec(memory_space=pltpu.SMEM),
            pl.BlockSpec(memory_space=pl.ANY),
            vmem,
            vmem,
        ],
        out_specs=vmem,
        scratch_shapes=[
            pltpu.VMEM((units, depth_count, samples, unit_rows, cols), jnp.int32),
            pltpu.VMEM((units, others, 4, unit_rows, cols), jnp.float32),
            pltpu.VMEM((units, 4, unit_rows, cols), jnp.float32),
            pltpu.VMEM((units, others, 4, unit_rows, cols), jnp.float32),
            pltpu.VMEM((units, owners, 4, rows_each, cols), jnp.float32),
            pltpu.SemaphoreType.DMA((units, depth_count)),
            pltpu.SemaphoreType.DMA((units, others)),
            pltpu.SemaphoreType.DMA((units, others)),
            pltpu.SemaphoreType.DMA((tile_count,)),
            pltpu.SemaphoreType.DMA((tile_count,)),
            pltpu.SemaphoreType.REGULAR,
            pltpu.SemaphoreType.REGULAR,
        ],
        compiler_params=pltpu.CompilerParams(collective_id=0, has_side_effects=True),
    )(slab_order.T, voxel_bins, colors, opacity)


def solution(mesh):
    placed = (P("depth", None, "screen"), P(), P(), P())
    return jax.shard_map(
        local,
        mesh=mesh,
        in_specs=placed,
        out_specs=P(None, ("depth", "screen"), None),
        check_vma=False,
    )
```

```python
import functools

import jax
import jax.numpy as jnp
from jax import lax
from jax.experimental import pallas as pl
from jax.experimental.pallas import tpu as pltpu
from jax.sharding import PartitionSpec as P

extinction = 3.0
lanes = 128
MESH = pl.DeviceIdType.MESH


def flip(index, mask, count):
    result = index
    bit = 1
    while bit < count:
        if isinstance(mask, int):
            if mask & bit:
                result = result + bit * (1 - 2 * lax.rem(lax.div(index, bit), 2))
        else:
            mine = lax.rem(lax.div(index, bit), 2)
            other = lax.rem(lax.div(mask, bit), 2)
            result = result + bit * other * (1 - 2 * mine)
        bit *= 2
    return result


def kernel(
    sizes,
    order_ref,
    bins_hbm,
    colors_ref,
    opacity_ref,
    out_ref,
    bins,
    sent,
    own,
    arrived,
    merged,
    bins_sem,
    send_sem,
    recv_sem,
    row_send_sem,
    row_recv_sem,
    ready_sem,
    go_sem,
):
    depth_count, tile_count, samples, unit_rows, units, owners, rows_each, cols, rate = sizes
    depth = lax.axis_index("depth")
    tile = lax.axis_index("screen")
    own_unit = lax.div(tile, owners)
    own_place = lax.rem(tile, owners)
    steps = list(range(units - 1, -1, -1))
    peers = [depth_count - 1] + list(range(1, depth_count - 1)) + [0]

    barrier = pltpu.get_barrier_semaphore()
    hub = depth == 0
    for mask in range(1, depth_count):
        peer = flip(depth, mask, depth_count)

        @pl.when(peer != 0)
        def _():
            pl.semaphore_signal(barrier, inc=1, device_id=(peer, tile), device_id_type=MESH)

    def meet_depth():
        @pl.when(jnp.logical_not(hub))
        def _():
            pl.semaphore_wait(barrier, depth_count - 1)
            pl.semaphore_signal(ready_sem, inc=1, device_id=(0, tile), device_id_type=MESH)

        @pl.when(hub)
        def _():
            pl.semaphore_wait(ready_sem, depth_count - 1)
            for mask in range(1, tile_count):
                pl.semaphore_signal(
                    barrier,
                    inc=1,
                    device_id=(0, flip(tile, mask, tile_count)),
                    device_id_type=MESH,
                )

    def meet_tiles():
        @pl.when(hub)
        def _():
            pl.semaphore_wait(barrier, tile_count - 1)
            for mask in range(1, depth_count):
                pl.semaphore_signal(go_sem, inc=1, device_id=(mask, tile), device_id_type=MESH)

        @pl.when(jnp.logical_not(hub))
        def _():
            pl.semaphore_wait(go_sem, 1)

    def fetch(step, mask):
        row = (flip(depth, mask, depth_count) * units + flip(own_unit, step, units)) * unit_rows
        row = pl.multiple_of(row, unit_rows)
        return pltpu.make_async_copy(
            bins_hbm.at[:, pl.ds(row, unit_rows), :],
            bins.at[step, mask],
            bins_sem.at[step, mask],
        )

    for step in steps:
        for mask in peers:
            if mask:
                fetch(step, mask).start()
    for step in steps:
        fetch(step, 0).start()

    density = opacity_ref[...].astype(jnp.float32).reshape(1, -1)
    weight = 1.0 - jnp.exp(-rate * density)
    shades = weight * colors_ref[...].astype(jnp.float32)
    table = [shades[c : c + 1] for c in range(3)] + [weight]
    bin_count = weight.shape[1]
    parts = [
        [jnp.broadcast_to(row[:, at : at + lanes], (8, lanes)) for at in range(0, bin_count, lanes)]
        for row in table
    ]

    def march(step, mask, target):
        for row in range(0, unit_rows, 8):
            for col in range(0, cols, lanes):
                clear = None
                total = None
                for j in range(samples):
                    index = bins[step, mask, j, row : row + 8, col : col + lanes]
                    low = lax.rem(index, lanes) if lanes & (lanes - 1) else index & (lanes - 1)
                    values = []
                    for part in parts:
                        value = jnp.take_along_axis(part[0], low, axis=1, mode="promise_in_bounds")
                        for n in range(1, len(part)):
                            other = jnp.take_along_axis(
                                part[n], low, axis=1, mode="promise_in_bounds"
                            )
                            value = jnp.where(index >= n * lanes, other, value)
                        values.append(value)
                    if total is None:
                        total = values
                        clear = 1.0 - values[3]
                    else:
                        seen = clear * values[3]
                        total = [t + clear * v for t, v in zip(total[:3], values[:3])] + [
                            total[3] + seen
                        ]
                        clear = clear - seen
                for c in range(4):
                    target[c, row : row + 8, col : col + lanes] = total[c]

    def send(step, mask):
        return pltpu.make_async_remote_copy(
            src_ref=sent.at[step, mask - 1],
            dst_ref=arrived.at[step, mask - 1],
            send_sem=send_sem.at[step, mask - 1],
            recv_sem=recv_sem.at[step, mask - 1],
            device_id=(flip(depth, mask, depth_count), tile),
            device_id_type=MESH,
        )

    def send_row(step, low):
        mask = step * owners + low
        place = flip(own_place, low, owners)
        there = pl.ds(pl.multiple_of(tile * cols, lanes), cols)
        return pltpu.make_async_remote_copy(
            src_ref=merged.at[step, place],
            dst_ref=out_ref.at[:, :, there],
            send_sem=row_send_sem.at[mask],
            recv_sem=row_recv_sem.at[mask],
            device_id=(depth, flip(tile, mask, tile_count)),
            device_id_type=MESH,
        )

    def take_row(mask):
        here = pl.ds(pl.multiple_of(flip(tile, mask, tile_count) * cols, lanes), cols)
        return pltpu.make_async_remote_copy(
            src_ref=merged.at[0, 0],
            dst_ref=out_ref.at[:, :, here],
            send_sem=row_send_sem.at[mask],
            recv_sem=row_recv_sem.at[mask],
            device_id=(depth, flip(tile, mask, tile_count)),
            device_id_type=MESH,
        )

    def feed(n):
        step = units - 1 - n
        for mask in peers:
            if mask:
                fetch(step, mask).wait()
                march(step, mask, sent.at[step, mask - 1])

        @pl.when(n == 0)
        def _():
            meet_depth()

        for mask in peers:
            if mask:
                send(step, mask).start()

    place_of = [order_ref[flip(depth, mask, depth_count), tile] for mask in range(depth_count)]
    ahead = [
        [jnp.where(place_of[j] < place_of[i], 1.0, 0.0) for j in range(depth_count)]
        for i in range(depth_count)
    ]

    def blend(n):
        step = units - 1 - n
        fetch(step, 0).wait()
        march(step, 0, own.at[step])

        @pl.when(n == 0)
        def _():
            meet_tiles()

        for mask in peers:
            if mask:
                send(step, mask).wait_recv()
        for row in range(0, unit_rows, 8):
            for col in range(0, cols, lanes):
                window = (slice(row, row + 8), slice(col, col + lanes))
                pieces = [
                    own[(step, slice(None)) + window]
                    if mask == 0
                    else arrived[(step, mask - 1, slice(None)) + window]
                    for mask in range(depth_count)
                ]
                total = None
                for i in range(depth_count):
                    front = None
                    for j in range(depth_count):
                        if j != i:
                            passed = 1.0 - ahead[i][j] * pieces[j][3]
                            front = passed if front is None else front * passed
                    lit = [pieces[i][c] if front is None else pieces[i][c] * front for c in range(4)]
                    total = lit if total is None else [t + v for t, v in zip(total, lit)]
                for c in range(4):
                    if owners == 1:
                        merged[step, 0, c, row : row + 8, col : col + lanes] = total[c]
                    else:
                        for place in range(owners):
                            merged[step, place, c, :, col : col + lanes] = total[c][
                                place * rows_each : (place + 1) * rows_each
                            ]
        for low in range(owners - 1, 0, -1):
            send_row(step, low).start()

        @pl.when(step > 0)
        def _():
            send_row(step, 0).start()

    lag = min(4, units)

    def advance(n, carry):
        @pl.when(n < units)
        def _():
            feed(n)

        @pl.when(n >= lag)
        def _():
            blend(n - lag)

        return carry

    lax.fori_loop(0, units + lag, advance, 0)
    here = pl.ds(pl.multiple_of(tile * cols, lanes), cols)
    out_ref[:, :, here] = merged[0, own_place]

    for mask in range(tile_count - 1, 0, -1):
        take_row(mask).wait_recv()
    for step in steps:
        for mask in range(1, depth_count):
            send(step, mask).wait_send()
    for mask in range(1, tile_count):
        send_row(mask // owners, mask % owners).wait_send()


def local(voxel_bins, colors, opacity, slab_order):
    depth_count = lax.axis_size("depth")
    tile_count = lax.axis_size("screen")
    samples, row_count, cols = voxel_bins.shape
    rows_each = row_count // (depth_count * tile_count)
    unit_rows = max(8, rows_each)
    owners = unit_rows // rows_each
    units = tile_count // owners
    rate = extinction / (samples * depth_count)
    sizes = (depth_count, tile_count, samples, unit_rows, units, owners, rows_each, cols, rate)
    others = depth_count - 1
    vmem = pl.BlockSpec(memory_space=pltpu.VMEM)
    return pl.pallas_call(
        functools.partial(kernel, sizes),
        out_shape=pltpu.VMEM((4, rows_each, cols * tile_count), jnp.float32),
        in_specs=[
            pl.BlockSpec(memory_space=pltpu.SMEM),
            pl.BlockSpec(memory_space=pl.ANY),
            vmem,
            vmem,
        ],
        out_specs=vmem,
        scratch_shapes=[
            pltpu.VMEM((units, depth_count, samples, unit_rows, cols), jnp.int32),
            pltpu.VMEM((units, others, 4, unit_rows, cols), jnp.float32),
            pltpu.VMEM((units, 4, unit_rows, cols), jnp.float32),
            pltpu.VMEM((units, others, 4, unit_rows, cols), jnp.float32),
            pltpu.VMEM((units, owners, 4, rows_each, cols), jnp.float32),
            pltpu.SemaphoreType.DMA((units, depth_count)),
            pltpu.SemaphoreType.DMA((units, others)),
            pltpu.SemaphoreType.DMA((units, others)),
            pltpu.SemaphoreType.DMA((tile_count,)),
            pltpu.SemaphoreType.DMA((tile_count,)),
            pltpu.SemaphoreType.REGULAR,
            pltpu.SemaphoreType.REGULAR,
        ],
        compiler_params=pltpu.CompilerParams(collective_id=0, has_side_effects=True),
    )(slab_order.T, voxel_bins, colors, opacity)


def solution(mesh):
    placed = (P("depth", None, "screen"), P(), P(), P())
    return jax.shard_map(
        local,
        mesh=mesh,
        in_specs=placed,
        out_specs=P(None, ("depth", "screen"), None),
        check_vma=False,
    )
```
